32 devices in a mesh: batch: 4 (over x, core), seq: 8 (over z, y).
Axes of the slice: x: 2, y: 2, z: 4, core: 2. Of those that a mesh axis runs over, the one named last changes fastest.
Arguments:
- query: bfloat16 [8, 64, 128], P('batch'), may hold values from -300 to 300
- cache_keys: bfloat16 [8, 16384, 512], P('batch', 'seq'), may hold values from -6 to 6
- cache_values: bfloat16 [8, 16384, 512], P('batch', 'seq'), may hold values from -6 to 6
- new_keys: bfloat16 [8, 512], P('batch'), may hold values from -6 to 6
- new_values: bfloat16 [8, 512], P('batch'), may hold values from -6 to 6
- key_up: bfloat16 [512, 1024], P('seq'), may hold values from -0.25 to 0.25
- value_up: bfloat16 [512, 1024], P('seq'), may hold values from -0.25 to 0.25
- out_weight: bfloat16 [8192, 8192], P('seq', 'batch'), may hold values from -0.5 to 0.5
- lengths: int32 [8], P('batch'), may hold values from 128 to 16384, as said below
Outputs:
- mixed: bfloat16 [8, 8192], P('seq', 'batch')
The draws below stay inside these ranges and needn't reach their ends.
Inputs may be any that keep to these rules, and one draw needn't show every extreme that they name: `lengths`: every length is a multiple of 128, at least 128; some sequence fills all 16384 slots. Slots at or beyond a sequence's length hold arbitrary finite entries that must not affect the result.
All inputs are finite; a program needn't handle non-finite values.
Results may differ from the reference program's by a relative error of at most 0.019.
Values may be sent and summed in bfloat16 or wider, within the bound.
A program may use at most 64 MiB of HBM per device.

```python
import jax
import jax.numpy as jnp
from jax import lax

D = 8192
H = 64
KV = 8
DH = 128
R = 512
BLOCK = 128
BATCH = 8
NTOK = 16384


def draw_query(key, part):
    base = jax.random.truncated_normal(key, -5.0, 5.0, (BATCH, H, DH), jnp.float32)
    values = base * 2.25
    return values.astype(jnp.bfloat16)


def draw_lengths(key, part):
    blocks = NTOK // BLOCK
    counts = jax.random.randint(key, (BATCH,), 1, blocks + 1)
    filled = jax.random.randint(jax.random.fold_in(key, 3), (), 0, BATCH)
    counts = jnp.where(jnp.arange(BATCH) == filled, blocks, counts)
    return (counts * BLOCK).astype(jnp.int32)


def level_of(rng, extent, shards, least, largest):
    factor_of, own = 1.0, jax.random.fold_in(rng, 6)
    for axis_at, blocks in shards:
        heights = jnp.exp(jax.random.uniform(jax.random.fold_in(own, axis_at), (blocks,), jnp.float32, least / len(shards), largest / len(shards)))
        factor_of = factor_of * jnp.repeat(heights, extent[axis_at] // blocks).reshape([-1 if axis == axis_at else 1 for axis in range(len(extent))])
    return factor_of


def noise(stream_key, dims, deviation, reach, shards=(), held_as=jnp.bfloat16):
    drawn = deviation * jax.random.normal(stream_key, dims, jnp.float32)
    if shards:
        drawn = drawn * level_of(stream_key, dims, shards, -0.22, 0.18)
    return jnp.clip(drawn, -reach, reach).astype(held_as)


def setup_inputs(seed: int = 0) -> dict:
    key_of = jax.random.split(jax.random.key(seed), 10)
    query = draw_query(jax.random.fold_in(key_of[9], 71), 0)
    cache_keys = noise(key_of[1], (BATCH, NTOK, R), 1.0, 6.0, ((0, 4), (1, 8)))
    cache_values = noise(key_of[2], (BATCH, NTOK, R), 1.0, 6.0, ((0, 4), (1, 8)))
    new_keys = noise(key_of[3], (BATCH, R), 1.0, 6.0, ((0, 4),))
    new_values = noise(key_of[4], (BATCH, R), 1.0, 6.0, ((0, 4),))
    key_up = noise(key_of[5], (R, KV * DH), R ** -0.5, 0.25, ((0, 8),))
    value_up = noise(key_of[6], (R, KV * DH), R ** -0.5, 0.25, ((0, 8),))
    out_weight = noise(key_of[7], (H * DH, D), DH ** -0.5, 0.5, ((0, 8), (1, 4)))
    lengths = draw_lengths(jax.random.fold_in(key_of[9], 71), 0)
    return dict(query=query, cache_keys=cache_keys, cache_values=cache_values, new_keys=new_keys, new_values=new_values, key_up=key_up, value_up=value_up, out_weight=out_weight, lengths=lengths)


def reference(query, cache_keys, cache_values, new_keys, new_values, key_up, value_up, out_weight, lengths):
    highest = lax.Precision.HIGHEST
    key_wide = key_up.astype(jnp.float32).reshape(R, KV, DH)
    value_wide = value_up.astype(jnp.float32).reshape(R, KV, DH)
    score_scale_factor = DH ** -0.5
    positions = jnp.arange(NTOK, dtype=jnp.int32)

    def per_sequence(items):
        query_row, keys_row, values_row, new_key_row, new_value_row, length = items
        grouped = query_row.astype(jnp.float32).reshape(KV, H // KV, DH)
        query_latent = jnp.einsum("kgd,rkd->kgr", grouped, key_wide, precision=highest)
        scores = jnp.einsum("kgr,lr->kgl", query_latent, keys_row.astype(jnp.float32), precision=highest) * score_scale_factor
        live_slots = positions < length
        scores = jnp.where(live_slots[None, None, :], scores, -jnp.inf)
        fresh_key_row = jnp.einsum("r,rkd->kd", new_key_row.astype(jnp.float32), key_wide, precision=highest)
        new_value = jnp.einsum("r,rkd->kd", new_value_row.astype(jnp.float32), value_wide, precision=highest)
        current_token_score = jnp.einsum("kgd,kd->kg", grouped, fresh_key_row, precision=highest) * score_scale_factor
        upper_limit = jnp.maximum(jnp.max(scores, axis=-1), current_token_score)
        softmax_terms = jnp.exp(scores - upper_limit[..., None])
        own_weight = jnp.exp(current_token_score - upper_limit)
        denominator = jnp.sum(softmax_terms, axis=-1) + own_weight
        latent_sum = jnp.einsum("kgl,lr->kgr", softmax_terms, values_row.astype(jnp.float32), precision=highest)
        totals = jnp.einsum("kgr,rkd->kgd", latent_sum, value_wide, precision=highest)
        totals = totals + own_weight[..., None] * new_value[:, None, :]
        return (totals / denominator[..., None]).reshape(H * DH).astype(jnp.bfloat16)

    attended = lax.map(per_sequence, (query, cache_keys, cache_values, new_keys, new_values, lengths))
    return jnp.dot(attended, out_weight, preferred_element_type=jnp.float32).astype(jnp.bfloat16)
```

```python
import functools

import jax
import jax.numpy as jnp
from jax import lax
from jax.experimental import pallas as pl
from jax.experimental.pallas import tpu as pltpu
from jax.sharding import PartitionSpec as P

NEGATIVE = -1e30
TOP_PRECISION = lax.Precision.HIGHEST
MESH = pl.DeviceIdType.MESH
NT = (((1,), (1,)), ((), ()))
NN = (((1,), (0,)), ((), ()))
F32 = jnp.float32
BF16 = jnp.bfloat16


def split_halves(x):
    head = x.astype(BF16)
    rest = (x - head.astype(F32)).astype(BF16)
    return jnp.concatenate([head, rest], axis=0)


def split_dot(x, y, dims):
    rows = x.shape[0]
    both = lax.dot_general(split_halves(x), y, dims, preferred_element_type=F32)
    return both[:rows] + both[rows:]


def step_kernel(
    ns, nb, lengths, query, keys, values, new_k, new_v, key_up, value_up, out_w, out,
    kbuf, vbuf, wbuf, qin, ku, nk, nv, qs, qfull, vcol, os, orecv, mls, mlrecv, att, ps, pr,
    lsem, qsend, qrecv, vsend, vrecv, osend, orcv, msend, mrcv, asend, arcv, psend, prcv,
):
    me = lax.axis_index("seq")
    mb = lax.axis_index("batch")
    seqs, heads, dh = qin.shape
    cache_len = kbuf.shape[1]
    rl = ku.shape[0]
    hl = heads // ns
    kv = ku.shape[1] // dh
    group = heads // kv
    rows = seqs * hl
    scale = dh ** (-0.5)

    local = [
        pltpu.make_async_copy(query, qin, lsem.at[0]),
        pltpu.make_async_copy(key_up, ku, lsem.at[1]),
        pltpu.make_async_copy(new_k, nk, lsem.at[2]),
        pltpu.make_async_copy(new_v, nv, lsem.at[3]),
        pltpu.make_async_copy(
            value_up.at[:, pl.ds(pl.multiple_of(me * dh, 128), dh)],
            vcol.at[pl.ds(pl.multiple_of(me * rl, 8), rl)],
            lsem.at[4],
        ),
        pltpu.make_async_copy(keys.at[0], kbuf.at[0], lsem.at[5]),
        pltpu.make_async_copy(keys.at[1], kbuf.at[1], lsem.at[6]),
        pltpu.make_async_copy(values.at[0], vbuf.at[0], lsem.at[7]),
        pltpu.make_async_copy(values.at[1], vbuf.at[1], lsem.at[8]),
        pltpu.make_async_copy(out_w, wbuf, lsem.at[9]),
    ]
    for copy in local:
        copy.start()

    barrier = pltpu.get_barrier_semaphore()
    for d in range(1, ns):
        pl.semaphore_signal(
            barrier, inc=1, device_id={"seq": lax.rem(me + d, ns)}, device_id_type=MESH
        )
    for d in range(1, nb):
        pl.semaphore_signal(
            barrier, inc=1, device_id={"batch": lax.rem(mb + d, nb)}, device_id_type=MESH
        )

    local[0].wait()
    local[1].wait()
    low = lax.broadcasted_iota(jnp.int32, (group, 2 * rl), 1) < rl
    for k in range(kv):
        part = ku[:, k * dh : (k + 1) * dh]
        twice = jnp.concatenate([part, part], axis=0)
        asked = jnp.concatenate(
            [qin[b, k * group : (k + 1) * group, :].astype(F32) for b in range(seqs)], axis=0
        ).astype(BF16)
        got = lax.dot_general(asked, twice, NT, preferred_element_type=F32)
        qs[me, k * group : (k + 1) * group, :] = jnp.where(low, got[:group], got[group:])

    pl.semaphore_wait(barrier, ns - 1 + nb - 1)

    def hop(src, dst, send, recv, d, axis, target):
        return pltpu.make_async_remote_copy(
            src_ref=src, dst_ref=dst, send_sem=send.at[d], recv_sem=recv.at[d],
            device_id={axis: target}, device_id_type=MESH,
        )

    started = []

    def send_all(count, index, axis, src_of, dst, send, recv):
        for d in range(1, count):
            target = lax.rem(index + d, count)
            copy = hop(src_of(target), dst(index), send, recv, d, axis, target)
            copy.start()
            started.append(copy)

    def receive(count, index, axis, src_of, dst, send, recv, d):
        source = lax.rem(index + count - d, count)
        hop(src_of(source), dst(source), send, recv, d, axis, source).wait_recv()

    q_args = (ns, me, "seq", lambda t: qs.at[me], lambda s: qs.at[s], qsend, qrecv)
    send_all(*q_args)

    for d in range(1, ns):
        receive(*q_args, d)

    v_args = (
        ns, me, "seq",
        lambda t: value_up.at[:, pl.ds(pl.multiple_of(t * dh, 128), dh)],
        lambda s: vcol.at[pl.ds(pl.multiple_of(s * rl, 8), rl)],
        vsend, vrecv,
    )
    send_all(*v_args)

    wide = lax.broadcasted_iota(jnp.int32, (heads, 2 * rl), 1) < rl
    for pair in range(ns // 2):
        even, odd = qs[2 * pair], qs[2 * pair + 1]
        lanes = slice(pair * 2 * rl, (pair + 1) * 2 * rl)
        qfull[0, :, lanes] = jnp.where(wide, even, pltpu.roll(odd, rl, 1))
        qfull[1, :, lanes] = jnp.where(wide, pltpu.roll(even, rl, 1), odd)

    positions = me * cache_len + lax.broadcasted_iota(jnp.int32, (1, cache_len), 1)
    sums, tops, totals = [], [], []
    for b in range(seqs):
        live = positions < lengths[b]
        local[5 + b].wait()
        scores = split_dot(qfull[b], kbuf[b], NT) * scale
        scores = jnp.where(live, scores, NEGATIVE)
        top = jnp.max(scores, axis=1, keepdims=True)
        terms = jnp.where(live, jnp.exp(scores - top), 0.0)
        tops.append(top)
        totals.append(jnp.sum(terms, axis=1, keepdims=True))
        local[7 + b].wait()
        sums.append(split_dot(terms, vbuf[b], NN))

    quarter = lax.broadcasted_iota(jnp.int32, (hl, 128), 1) // 32
    for p in range(ns):
        span = slice(p * hl, (p + 1) * hl)
        os[p] = jnp.concatenate([x[span] for x in sums], axis=0).astype(BF16)
        mls[p] = jnp.where(
            quarter == 0, tops[0][span],
            jnp.where(
                quarter == 1, totals[0][span],
                jnp.where(quarter == 2, tops[1][span], totals[1][span]),
            ),
        )
    m_args = (ns, me, "seq", lambda t: mls.at[t], lambda s: mlrecv.at[s], msend, mrcv)
    o_args = (ns, me, "seq", lambda t: os.at[t], lambda s: orecv.at[s], osend, orcv)
    send_all(*m_args)
    send_all(*o_args)

    local[2].wait()
    local[3].wait()
    local[4].wait()
    mine = pl.ds(pl.multiple_of(me * hl, 8), hl)
    own_query = jnp.concatenate([qfull[b, mine, :] for b in range(seqs)], axis=0)

    def spread(ref):
        full = ref[...].astype(F32)
        return jnp.concatenate(
            [jnp.broadcast_to(full[b : b + 1], (hl, full.shape[1])) for b in range(seqs)], axis=0
        )

    own = jnp.sum(own_query * spread(nk), axis=1, keepdims=True) * scale
    fresh = spread(nv)

    def stats(x):
        return (
            jnp.concatenate([x[:, 0:1], x[:, 64:65]], axis=0),
            jnp.concatenate([x[:, 32:33], x[:, 96:97]], axis=0),
        )

    parts = [stats(mls[me])]
    for d in range(1, ns):
        receive(*m_args, d)
        parts.append(stats(mlrecv[lax.rem(me + ns - d, ns)]))
    limit = own
    for top, _ in parts:
        limit = jnp.maximum(limit, top)
    own_weight = jnp.exp(own - limit)
    latent = own_weight * fresh
    below = own_weight
    for d, (top, total) in enumerate(parts):
        factor = jnp.exp(top - limit)
        below = below + factor * total
        if d:
            receive(*o_args, d)
            block = orecv[lax.rem(me + ns - d, ns)]
        else:
            block = os[me]
        latent = latent + factor * block.astype(F32)
    for d in range(1, ns):
        receive(*v_args, d)
    attended = split_dot(latent, vcol[...], NN) / below
    att[pl.ds(pl.multiple_of(mb * rows, 8), rows), :] = attended.astype(BF16).astype(F32)

    def att_rows(i):
        return att.at[pl.ds(pl.multiple_of(i * rows, 8), rows)]

    a_args = (nb, mb, "batch", lambda t: att_rows(mb), att_rows, asend, arcv)
    send_all(*a_args)
    for d in range(1, nb):
        receive(*a_args, d)
    features = jnp.concatenate(
        [att[pl.ds(g, nb * seqs, stride=hl), :] for g in range(hl)], axis=1
    ).astype(BF16)
    local[9].wait()
    product = lax.dot_general(features, wbuf[...], NN, preferred_element_type=F32)
    for p in range(ns):
        ps[p] = product[p : p + 1]
    p_args = (ns, me, "seq", lambda t: ps.at[t], lambda s: pr.at[s], psend, prcv)
    send_all(*p_args)
    result = ps[me]
    for d in range(1, ns):
        receive(*p_args, d)
        result = result + pr[lax.rem(me + ns - d, ns)]
    out[...] = result.astype(out.dtype)
    for copy in started:
        copy.wait_send()


def fused_body(
    query, cache_keys, cache_values, new_keys, new_values, key_up, value_up, out_weight, lengths
):
    ns, nb = lax.axis_size("seq"), lax.axis_size("batch")
    seqs, cache_len, rank = cache_keys.shape
    heads, dh = query.shape[1:]
    hl = heads // ns
    width = out_weight.shape[1]
    sem = pltpu.SemaphoreType.DMA
    hbm = pl.BlockSpec(memory_space=pl.ANY)
    return pl.pallas_call(
        functools.partial(step_kernel, ns, nb),
        out_shape=jax.ShapeDtypeStruct((1, width), BF16),
        in_specs=[pl.BlockSpec(memory_space=pltpu.SMEM)] + [hbm] * 8,
        out_specs=pl.BlockSpec(memory_space=pltpu.VMEM),
        scratch_shapes=[
            pltpu.VMEM(cache_keys.shape, BF16),
            pltpu.VMEM(cache_values.shape, BF16),
            pltpu.VMEM(out_weight.shape, BF16),
            pltpu.VMEM(query.shape, BF16),
            pltpu.VMEM(key_up.shape, BF16),
            pltpu.VMEM(new_keys.shape, BF16),
            pltpu.VMEM(new_values.shape, BF16),
            pltpu.VMEM((ns, heads, seqs * key_up.shape[0]), F32),
            pltpu.VMEM((seqs, heads, rank), F32),
            pltpu.VMEM((rank, dh), BF16),
            pltpu.VMEM((ns, seqs * hl, rank), BF16),
            pltpu.VMEM((ns, seqs * hl, rank), BF16),
            pltpu.VMEM((ns, hl, 128), F32),
            pltpu.VMEM((ns, hl, 128), F32),
            pltpu.VMEM((nb * seqs * hl, dh), F32),
            pltpu.VMEM((ns, 1, width), F32),
            pltpu.VMEM((ns, 1, width), F32),
            sem((10,)),
        ]
        + [sem((ns,))] * 8
        + [sem((nb,))] * 2
        + [sem((ns,))] * 2,
        compiler_params=pltpu.CompilerParams(collective_id=0, has_side_effects=True),
        name="decode_step",
    )(
        lengths, query, cache_keys, cache_values, new_keys, new_values, key_up, value_up, out_weight
    )


def fits(mesh, query, cache_keys, key_up):
    ns, nb = mesh.shape["seq"], mesh.shape["batch"]
    heads, dh = query.shape[1:]
    kv = key_up.shape[1] // dh
    seqs = query.shape[0] // nb
    return (
        seqs == 2 and kv == ns and heads // kv == 8 and dh == 128
        and key_up.shape[0] // ns == 64 and query.shape[0] == ns
        and cache_keys.shape[1] // ns * cache_keys.shape[2] <= 2 ** 21
    )


def body(
    query, cache_keys, cache_values, new_keys, new_values, key_up, value_up, out_weight, lengths
):
    batch_rows, cache_len, rank_full = cache_keys.shape
    head_count, head_dimension = (query.shape[1], query.shape[2])
    kv_heads = key_up.shape[1] // head_dimension
    group_size = head_count // kv_heads
    score_scale_factor = head_dimension ** (-0.5)
    seq_index = lax.axis_index("seq")
    seq_count = lax.axis_size("seq")
    local_head_index = head_count // seq_count
    positions = seq_index * cache_len + lax.iota(jnp.int32, cache_len)
    live_mask = (positions[None, :] < lengths[:, None])[:, None, None, :]
    grouped = query.reshape(batch_rows, kv_heads, group_size, head_dimension)
    key_full, value_full = (
        lax.all_gather(key_up, "seq", axis=0, tiled=True),
        lax.all_gather(value_up, "seq", axis=0, tiled=True),
    )
    rebuilt_keys = jnp.dot(
        cache_keys.reshape(batch_rows * cache_len, rank_full),
        key_full,
        preferred_element_type=jnp.float32,
    ).reshape(batch_rows, cache_len, kv_heads, head_dimension)
    rebuilt_values = jnp.dot(
        cache_values.reshape(batch_rows * cache_len, rank_full),
        value_full,
        preferred_element_type=jnp.float32,
    ).reshape(batch_rows, cache_len, kv_heads, head_dimension)
    expanded_query = grouped.astype(jnp.float32)
    scores = (
        jnp.einsum("bkgd,blkd->bkgl", expanded_query, rebuilt_keys, precision=TOP_PRECISION)
        * score_scale_factor
    )
    fresh_key_row = jnp.dot(new_keys, key_full, preferred_element_type=jnp.float32).reshape(
        batch_rows, kv_heads, head_dimension
    )
    current_token_score = (
        jnp.einsum("phsu,phu->phs", expanded_query, fresh_key_row, precision=TOP_PRECISION)
        * score_scale_factor
    )
    new_value = jnp.dot(new_values, value_full, preferred_element_type=jnp.float32).reshape(
        batch_rows, kv_heads, head_dimension
    )
    scores = jnp.where(live_mask, scores, NEGATIVE)
    local_max = jnp.max(scores, axis=-1)
    upper_limit = jnp.maximum(lax.pmax(local_max, "seq"), current_token_score)
    softmax_terms = jnp.where(live_mask, jnp.exp(scores - upper_limit[..., None]), 0.0)
    denominator = jnp.sum(softmax_terms, axis=-1)
    totals = jnp.einsum("bkgl,blkd->bkgd", softmax_terms, rebuilt_values, precision=TOP_PRECISION)
    denominator, totals = (
        lax.psum(denominator.astype(jnp.bfloat16), "seq").astype(jnp.float32),
        lax.psum(totals.astype(jnp.bfloat16), "seq").astype(jnp.float32),
    )
    own_weight = jnp.exp(current_token_score - upper_limit)
    normalized = (totals + own_weight[..., None] * new_value[:, :, None, :]) / (
        denominator + own_weight
    )[..., None]
    normalized = normalized.reshape(batch_rows, head_count * head_dimension)
    width_local = local_head_index * head_dimension
    attended = lax.dynamic_slice_in_dim(normalized, seq_index * width_local, width_local, 1).astype(
        jnp.bfloat16
    )
    partial_out = jnp.dot(
        lax.all_gather(attended, "batch", axis=0, tiled=True),
        out_weight,
        preferred_element_type=jnp.float32,
    )
    return lax.psum_scatter(
        partial_out.astype(jnp.bfloat16), "seq", scatter_dimension=0, tiled=True
    )


def solution(mesh):
    placed = (
        P("batch", None, None),
        P("batch", "seq", None),
        P("batch", "seq", None),
        P("batch", None),
        P("batch", None),
        P("seq", None),
        P("seq", None),
        P("seq", "batch"),
        P("batch"),
    )

    def run(*args):
        chosen = fused_body if fits(mesh, args[0], args[1], args[5]) else body
        return jax.shard_map(
            chosen, mesh=mesh, in_specs=placed, out_specs=P("seq", "batch"), check_vma=False
        )(*args)

    return run
```

```python
import functools

import jax
import jax.numpy as jnp
from jax import lax
from jax.experimental import pallas as pl
from jax.experimental.pallas import tpu as pltpu
from jax.sharding import PartitionSpec as P

NEGATIVE = -1e30
TOP_PRECISION = lax.Precision.HIGHEST
MESH = pl.DeviceIdType.MESH
NT = (((1,), (1,)), ((), ()))
NN = (((1,), (0,)), ((), ()))
F32 = jnp.float32
BF16 = jnp.bfloat16


def split_halves(x):
    head = x.astype(BF16)
    rest = (x - head.astype(F32)).astype(BF16)
    return jnp.concatenate([head, rest], axis=0)


def split_dot(x, y, dims):
    rows = x.shape[0]
    both = lax.dot_general(split_halves(x), y, dims, preferred_element_type=F32)
    return both[:rows] + both[rows:]


def step_kernel(
    ns, nb, lengths, query, keys, values, new_k, new_v, key_up, value_up, out_w, out,
    kbuf, vbuf, wbuf, qin, ku, nk, nv, qs, qfull, vcol, os, orecv, att, ps, pr,
    lsem, qsend, qrecv, vsend, vrecv, osend, orcv, asend, arcv, psend, prcv,
):
    me = lax.axis_index("seq")
    mb = lax.axis_index("batch")
    seqs, heads, dh = qin.shape
    cache_len = kbuf.shape[1]
    rl = ku.shape[0]
    hl = heads // ns
    kv = ku.shape[1] // dh
    group = heads // kv
    rows = seqs * hl
    scale = dh ** (-0.5)

    local = [
        pltpu.make_async_copy(query, qin, lsem.at[0]),
        pltpu.make_async_copy(key_up, ku, lsem.at[1]),
        pltpu.make_async_copy(new_k, nk, lsem.at[2]),
        pltpu.make_async_copy(new_v, nv, lsem.at[3]),
        pltpu.make_async_copy(
            value_up.at[:, pl.ds(pl.multiple_of(me * dh, 128), dh)],
            vcol.at[pl.ds(pl.multiple_of(me * rl, 8), rl)],
            lsem.at[4],
        ),
        pltpu.make_async_copy(keys.at[0], kbuf.at[0], lsem.at[5]),
        pltpu.make_async_copy(keys.at[1], kbuf.at[1], lsem.at[6]),
        pltpu.make_async_copy(values.at[0], vbuf.at[0], lsem.at[7]),
        pltpu.make_async_copy(values.at[1], vbuf.at[1], lsem.at[8]),
        pltpu.make_async_copy(out_w, wbuf, lsem.at[9]),
    ]
    for copy in local:
        copy.start()

    barrier = pltpu.get_barrier_semaphore()
    for d in range(1, ns):
        pl.semaphore_signal(
            barrier, inc=1, device_id={"seq": lax.rem(me + d, ns)}, device_id_type=MESH
        )
    for d in range(1, nb):
        pl.semaphore_signal(
            barrier, inc=1, device_id={"batch": lax.rem(mb + d, nb)}, device_id_type=MESH
        )

    local[0].wait()
    local[1].wait()
    low = lax.broadcasted_iota(jnp.int32, (group, 2 * rl), 1) < rl
    for k in range(kv):
        part = ku[:, k * dh : (k + 1) * dh]
        twice = jnp.concatenate([part, part], axis=0)
        asked = jnp.concatenate(
            [qin[b, k * group : (k + 1) * group, :].astype(F32) for b in range(seqs)], axis=0
        ).astype(BF16)
        got = lax.dot_general(asked, twice, NT, preferred_element_type=F32)
        qs[me, k * group : (k + 1) * group, :] = jnp.where(low, got[:group], got[group:])

    pl.semaphore_wait(barrier, ns - 1 + nb - 1)

    def hop(src, dst, send, recv, d, axis, target):
        return pltpu.make_async_remote_copy(
            src_ref=src, dst_ref=dst, send_sem=send.at[d], recv_sem=recv.at[d],
            device_id={axis: target}, device_id_type=MESH,
        )

    started = []
    bits = [lax.rem(lax.div(me, 1 << i), 2) for i in range((ns - 1).bit_length())]

    def across(d):
        return sum((1 - x if d >> i & 1 else x) * (1 << i) for i, x in enumerate(bits))

    def send_all(order, partner, index, axis, src_of, dst, send, recv):
        for d in order:
            copy = hop(src_of(partner(d)), dst(index), send, recv, d, axis, partner(d))
            copy.start()
            started.append(copy)

    def receive(d, partner, axis, src_of, dst, send, recv):
        hop(src_of(partner(d)), dst(partner(d)), send, recv, d, axis, partner(d)).wait_recv()

    near, far = list(range(1, ns // 2)), list(range(ns // 2, ns))
    everyone = near + far
    q_src, q_dst = (lambda t: qs.at[me]), (lambda s: qs.at[s])
    send_all(everyone, across, me, "seq", q_src, q_dst, qsend, qrecv)

    wide = lax.broadcasted_iota(jnp.int32, (heads, 2 * rl), 1) < rl
    side = lax.div(me, ns // 2)
    half_rank = rl * ns // 2

    def gathered(half):
        for pair in range(ns // 4):
            even = qs[half * (ns // 2) + 2 * pair]
            odd = qs[half * (ns // 2) + 2 * pair + 1]
            lanes = slice(pair * 2 * rl, (pair + 1) * 2 * rl)
            qfull[0, half, :, lanes] = jnp.where(wide, even, pltpu.roll(odd, rl, 1))
            qfull[1, half, :, lanes] = jnp.where(wide, pltpu.roll(even, rl, 1), odd)

    def half_scores(b, half):
        columns = pl.ds(pl.multiple_of(half * half_rank, 128), half_rank)
        return split_dot(qfull[b, half], kbuf[b, :, columns], NT)

    for d in near:
        receive(d, across, "seq", q_src, q_dst, qsend, qrecv)
    gathered(side)
    early = []
    for b in range(seqs):
        local[5 + b].wait()
        early.append(half_scores(b, side))
    for d in far:
        receive(d, across, "seq", q_src, q_dst, qsend, qrecv)
    gathered(1 - side)

    v_src = lambda t: value_up.at[:, pl.ds(pl.multiple_of(t * dh, 128), dh)]
    v_dst = lambda s: vcol.at[pl.ds(pl.multiple_of(s * rl, 8), rl)]
    send_all(everyone, across, me, "seq", v_src, v_dst, vsend, vrecv)

    positions = me * cache_len + lax.broadcasted_iota(jnp.int32, (1, cache_len), 1)
    lane = lax.broadcasted_iota(jnp.int32, (heads, 128), 1)
    o_args = []
    for b in range(seqs):
        live = positions < lengths[b]
        scores = (early[b] + half_scores(b, 1 - side)) * scale
        scores = jnp.where(live, scores, NEGATIVE)
        top = jnp.max(scores, axis=1, keepdims=True)
        terms = jnp.where(live, jnp.exp(scores - top), 0.0)
        total = jnp.sum(terms, axis=1, keepdims=True)
        local[7 + b].wait()
        sums = split_dot(terms, vbuf[b], NN)
        pieces = jnp.zeros((heads, 128), F32)
        for at, value in ((0, top), (3, total)):
            for k in range(3):
                piece = value.astype(BF16).astype(F32)
                pieces = jnp.where(lane == at + k, piece, pieces)
                value = value - piece
        packed = jnp.concatenate([sums, pieces], axis=1)
        for p in range(ns):
            os[b, p] = packed[p * hl : (p + 1) * hl].astype(BF16)
        o_args.append(
            (
                "seq", lambda t, b=b: os.at[b, t], lambda s, b=b: orecv.at[b, s],
                osend.at[b], orcv.at[b],
            )
        )
        send_all(everyone, across, me, *o_args[b])
        orecv[b, me] = os[b, me]

    local[2].wait()
    local[3].wait()
    local[4].wait()
    mine = pl.ds(pl.multiple_of(me * hl, 8), hl)
    own_query = jnp.concatenate(
        [
            jnp.concatenate([qfull[b, half, mine, :] for half in range(2)], axis=1)
            for b in range(seqs)
        ],
        axis=0,
    )

    def spread(ref):
        full = ref[...].astype(F32)
        return jnp.concatenate(
            [jnp.broadcast_to(full[b : b + 1], (hl, full.shape[1])) for b in range(seqs)], axis=0
        )

    own = jnp.sum(own_query * spread(nk), axis=1, keepdims=True) * scale
    fresh = spread(nv)

    rank = nk.shape[1]
    latents, belows = [], []
    for b in range(seqs):
        for d in near + far:
            receive(d, across, *o_args[b])
        span = slice(b * hl, (b + 1) * hl)
        notes = orecv[b, :, :, rank:].astype(F32)
        top = notes[:, :, 0:1] + notes[:, :, 1:2] + notes[:, :, 2:3]
        total = notes[:, :, 3:4] + notes[:, :, 4:5] + notes[:, :, 5:6]
        limit = jnp.maximum(jnp.max(top, axis=0), own[span])
        factor = jnp.exp(top - limit[None])
        own_weight = jnp.exp(own[span] - limit)
        latent = own_weight * fresh[span]
        for p in range(ns):
            latent = latent + factor[p] * orecv[b, p, :, :rank].astype(F32)
        latents.append(latent)
        belows.append(own_weight + jnp.sum(factor * total, axis=0))
    latent = jnp.concatenate(latents, axis=0)
    below = jnp.concatenate(belows, axis=0)
    for d in near + far:
        receive(d, across, "seq", v_src, v_dst, vsend, vrecv)
    attended = split_dot(latent, vcol[...], NN) / below
    att[pl.ds(pl.multiple_of(mb * rows, 8), rows), :] = attended.astype(BF16).astype(F32)

    def att_rows(i):
        return att.at[pl.ds(pl.multiple_of(i * rows, 8), rows)]

    def turned(d):
        return lax.rem(mb + d, nb)

    def turned_back(d):
        return lax.rem(mb + nb - d, nb)

    a_src = lambda t: att_rows(mb)
    send_all(range(1, nb), turned, mb, "batch", a_src, att_rows, asend, arcv)
    for d in range(1, nb):
        receive(d, turned_back, "batch", a_src, att_rows, asend, arcv)
    features = jnp.concatenate(
        [att[pl.ds(g, nb * seqs, stride=hl), :] for g in range(hl)], axis=1
    ).astype(BF16)
    local[9].wait()
    product = lax.dot_general(features, wbuf[...], NN, preferred_element_type=F32)
    for p in range(ns):
        ps[p] = product[p : p + 1].astype(ps.dtype)
    p_src, p_dst = (lambda t: ps.at[t]), (lambda s: pr.at[s])
    send_all(everyone, across, me, "seq", p_src, p_dst, psend, prcv)
    pr[me] = ps[me]
    for d in near + far:
        receive(d, across, "seq", p_src, p_dst, psend, prcv)
    result = pr[0].astype(F32)
    for p in range(1, ns):
        result = result + pr[p].astype(F32)
    out[...] = result.astype(out.dtype)
    for copy in started:
        copy.wait_send()


def fused_body(
    query, cache_keys, cache_values, new_keys, new_values, key_up, value_up, out_weight, lengths
):
    ns, nb = lax.axis_size("seq"), lax.axis_size("batch")
    seqs, cache_len, rank = cache_keys.shape
    heads, dh = query.shape[1:]
    hl = heads // ns
    width = out_weight.shape[1]
    sem = pltpu.SemaphoreType.DMA
    hbm = pl.BlockSpec(memory_space=pl.ANY)
    return pl.pallas_call(
        functools.partial(step_kernel, ns, nb),
        out_shape=jax.ShapeDtypeStruct((1, width), BF16),
        in_specs=[pl.BlockSpec(memory_space=pltpu.SMEM)] + [hbm] * 8,
        out_specs=pl.BlockSpec(memory_space=pltpu.VMEM),
        scratch_shapes=[
            pltpu.VMEM(cache_keys.shape, BF16),
            pltpu.VMEM(cache_values.shape, BF16),
            pltpu.VMEM(out_weight.shape, BF16),
            pltpu.VMEM(query.shape, BF16),
            pltpu.VMEM(key_up.shape, BF16),
            pltpu.VMEM(new_keys.shape, BF16),
            pltpu.VMEM(new_values.shape, BF16),
            pltpu.VMEM((ns, heads, seqs * key_up.shape[0]), F32),
            pltpu.VMEM((seqs, 2, heads, rank // 2), F32),
            pltpu.VMEM((rank, dh), BF16),
            pltpu.VMEM((seqs, ns, hl, rank + 128), BF16),
            pltpu.VMEM((seqs, ns, hl, rank + 128), BF16),
            pltpu.VMEM((nb * seqs * hl, dh), F32),
            pltpu.VMEM((ns, 1, width), BF16),
            pltpu.VMEM((ns, 1, width), BF16),
            sem((10,)),
        ]
        + [sem((ns,))] * 4
        + [sem((seqs, ns))] * 2
        + [sem((nb,))] * 2
        + [sem((ns,))] * 2,
        compiler_params=pltpu.CompilerParams(collective_id=0, has_side_effects=True),
        name="decode_step",
    )(
        lengths, query, cache_keys, cache_values, new_keys, new_values, key_up, value_up, out_weight
    )


def fits(mesh, query, cache_keys, key_up):
    ns, nb = mesh.shape["seq"], mesh.shape["batch"]
    heads, dh = query.shape[1:]
    kv = key_up.shape[1] // dh
    seqs = query.shape[0] // nb
    return (
        seqs == 2 and kv == ns and heads // kv == 8 and dh == 128
        and key_up.shape[0] // ns == 64 and query.shape[0] == ns
        and cache_keys.shape[1] // ns * cache_keys.shape[2] <= 2 ** 21
    )


def body(
    query, cache_keys, cache_values, new_keys, new_values, key_up, value_up, out_weight, lengths
):
    batch_rows, cache_len, rank_full = cache_keys.shape
    head_count, head_dimension = (query.shape[1], query.shape[2])
    kv_heads = key_up.shape[1] // head_dimension
    group_size = head_count // kv_heads
    score_scale_factor = head_dimension ** (-0.5)
    seq_index = lax.axis_index("seq")
    seq_count = lax.axis_size("seq")
    local_head_index = head_count // seq_count
    positions = seq_index * cache_len + lax.iota(jnp.int32, cache_len)
    live_mask = (positions[None, :] < lengths[:, None])[:, None, None, :]
    grouped = query.reshape(batch_rows, kv_heads, group_size, head_dimension)
    key_full, value_full = (
        lax.all_gather(key_up, "seq", axis=0, tiled=True),
        lax.all_gather(value_up, "seq", axis=0, tiled=True),
    )
    rebuilt_keys = jnp.dot(
        cache_keys.reshape(batch_rows * cache_len, rank_full),
        key_full,
        preferred_element_type=jnp.float32,
    ).reshape(batch_rows, cache_len, kv_heads, head_dimension)
    rebuilt_values = jnp.dot(
        cache_values.reshape(batch_rows * cache_len, rank_full),
        value_full,
        preferred_element_type=jnp.float32,
    ).reshape(batch_rows, cache_len, kv_heads, head_dimension)
    expanded_query = grouped.astype(jnp.float32)
    scores = (
        jnp.einsum("bkgd,blkd->bkgl", expanded_query, rebuilt_keys, precision=TOP_PRECISION)
        * score_scale_factor
    )
    fresh_key_row = jnp.dot(new_keys, key_full, preferred_element_type=jnp.float32).reshape(
        batch_rows, kv_heads, head_dimension
    )
    current_token_score = (
        jnp.einsum("phsu,phu->phs", expanded_query, fresh_key_row, precision=TOP_PRECISION)
        * score_scale_factor
    )
    new_value = jnp.dot(new_values, value_full, preferred_element_type=jnp.float32).reshape(
        batch_rows, kv_heads, head_dimension
    )
    scores = jnp.where(live_mask, scores, NEGATIVE)
    local_max = jnp.max(scores, axis=-1)
    upper_limit = jnp.maximum(lax.pmax(local_max, "seq"), current_token_score)
    softmax_terms = jnp.where(live_mask, jnp.exp(scores - upper_limit[..., None]), 0.0)
    denominator = jnp.sum(softmax_terms, axis=-1)
    totals = jnp.einsum("bkgl,blkd->bkgd", softmax_terms, rebuilt_values, precision=TOP_PRECISION)
    denominator, totals = (
        lax.psum(denominator.astype(jnp.bfloat16), "seq").astype(jnp.float32),
        lax.psum(totals.astype(jnp.bfloat16), "seq").astype(jnp.float32),
    )
    own_weight = jnp.exp(current_token_score - upper_limit)
    normalized = (totals + own_weight[..., None] * new_value[:, :, None, :]) / (
        denominator + own_weight
    )[..., None]
    normalized = normalized.reshape(batch_rows, head_count * head_dimension)
    width_local = local_head_index * head_dimension
    attended = lax.dynamic_slice_in_dim(normalized, seq_index * width_local, width_local, 1).astype(
        jnp.bfloat16
    )
    partial_out = jnp.dot(
        lax.all_gather(attended, "batch", axis=0, tiled=True),
        out_weight,
        preferred_element_type=jnp.float32,
    )
    return lax.psum_scatter(
        partial_out.astype(jnp.bfloat16), "seq", scatter_dimension=0, tiled=True
    )


def solution(mesh):
    placed = (
        P("batch", None, None),
        P("batch", "seq", None),
        P("batch", "seq", None),
        P("batch", None),
        P("batch", None),
        P("seq", None),
        P("seq", None),
        P("seq", "batch"),
        P("batch"),
    )

    def run(*args):
        chosen = fused_body if fits(mesh, args[0], args[1], args[5]) else body
        return jax.shard_map(
            chosen, mesh=mesh, in_specs=placed, out_specs=P("seq", "batch"), check_vma=False
        )(*args)

    return run
```
